32 devices in a mesh: dp: 4 (over x, core), expert: 8 (over z, y).
Axes of the slice: x: 2, y: 2, z: 4, core: 2. Of those that a mesh axis runs over, the one named last changes fastest.
Arguments:
- queries: bfloat16 [2, 4, 8, 2048], P(None, 'dp', 'expert'), may hold values from -5 to 5
- cache_keys: bfloat16 [4, 8, 512, 512], P('dp', 'expert'), may hold values from -5 to 5
- cache_values: bfloat16 [4, 8, 512, 512], P('dp', 'expert'), may hold values from -6 to 6
- new_keys: bfloat16 [2, 4, 8, 512], P(None, 'dp', 'expert'), may hold values from -9 to 9
- new_values: bfloat16 [2, 4, 8, 512], P(None, 'dp', 'expert'), may hold values from -6 to 6
- cache_len: int32 [4, 8], P('dp', 'expert'), may hold values from 256 to 510, as said below
- o_proj: bfloat16 [2048, 4096], P(None, 'expert'), may hold values from -0.125 to 0.125
- residual_in: bfloat16 [2, 4, 8, 4096], P(None, 'dp', None, 'expert'), may hold values from -36 to 36
- norm_gain: float32 [4096], P('expert'), may hold values from 0.1 to 1.9
- router: float32 [4096, 8], P('expert'), may hold values from -0.09375 to 0.09375
- expert_gate: bfloat16 [8, 4096, 14336], P('expert', None, 'dp'), may hold values from -0.09375 to 0.09375
- expert_up: bfloat16 [8, 4096, 14336], P('expert', None, 'dp'), may hold values from -0.09375 to 0.09375
- expert_down: bfloat16 [8, 14336, 4096], P('expert', 'dp'), may hold values from -0.046875 to 0.046875
- routes: int32 [2, 4, 8, 2], replicated, may hold values from 0 to 7, all different within a row; in each aligned block of 8 rows (0 to 7, 8 to 15, ..., all dimensions but the last counted through in order) at most 4 rows name the same one
- answers: int32 [2, 4, 8], P(None, 'dp', 'expert'), may hold values from 0 to 127
- stop_mask: int32 [2, 4], P(None, 'dp'), may hold values 0 or 1
Outputs:
- residual_out: bfloat16 [2, 4, 8, 4096], P(None, 'dp', None, 'expert')
- vote_share: float32 [2, 4, 128], P(None, 'dp')
The draws below stay inside these ranges and needn't reach their ends.
Inputs may be any that keep to these rules, and one draw needn't show every extreme that they name: `cache_len`: some sequence uses exactly 510 cached positions. `routes`: each token names 2 different experts; in each step, the tokens of the 1 prompts of one index of dp (all their samples together) name one expert at most 4 times.
All inputs are finite; a program needn't handle non-finite values. No bound on the sum of `stop_mask` on one device may be relied on, other than what follows from the above.
Results may differ from the reference program's by a relative error of at most 0.0055.
Values may be sent and summed in bfloat16 or wider, within the bound.
No kernel may reach another device: no remote copies, remote signals or barrier semaphores. Data moves between devices by JAX's collectives and lax.ppermute only.
A program may use at most 192 MiB of HBM per device.

```python
import math
import jax
import jax.numpy as jnp
import numpy as np
from jax import lax

D = 4096
E = 8
TOP = 2
HD = 128
QH = 16
KVH = 4
FFW = 14336
STEPS = 2
ANSWERS = 128
CACHE = 512
PROMPT_DEV = 1
PROMPTS = 4
SAMPLES = 8
SPLIT = 1
CAP = 4


def draw_queries(key, part):
    noise_key = jax.random.fold_in(key, 3)
    full_shape = (STEPS, PROMPTS, SAMPLES, QH * HD)
    return jnp.clip(2.0 * jax.random.normal(noise_key, full_shape, jnp.float32), -5.0, 5.0).astype(jnp.bfloat16)


def draw_cache_keys(key, part):
    noise_key = jax.random.fold_in(key, 5)
    full_shape = (PROMPTS, SAMPLES, CACHE, KVH * HD)
    return jnp.clip(jax.random.normal(noise_key, full_shape, jnp.float32), -4.0, 4.0).astype(jnp.bfloat16)


def draw_residual_in(key, part):
    noise_key = jax.random.fold_in(jax.random.fold_in(key, 11), 0)
    full_shape = (STEPS, PROMPTS, SAMPLES, D)
    values = jnp.clip(jax.random.normal(noise_key, full_shape, jnp.float32), -4.0, 4.0)
    return values.astype(jnp.bfloat16)


def draw_cache_len(key, part):
    lengths = jax.random.randint(jax.random.fold_in(key, 13), (PROMPTS, SAMPLES), CACHE // 2, CACHE - STEPS + 1, dtype=jnp.int32)
    return lengths.at[0, 0].set(CACHE - STEPS)


def touch_ends(values, rng, least, top_value):
    spot = [jax.random.randint(jax.random.fold_in(rng, axis), (), 0, length) for axis, length in enumerate(values.shape)]
    widest = values.shape.index(max(values.shape))
    beside = spot[:widest] + [(spot[widest] + 1) % values.shape[widest]] + spot[widest + 1:]
    return values.at[tuple(spot)].set(least).at[tuple(beside)].set(top_value)


def block_levels(stream_key, shape, pieces, smallest, high):
    loudness = 1.0
    for position, parts in pieces:
        draws = jax.random.uniform(jax.random.fold_in(jax.random.fold_in(stream_key, 6), position), (parts,), jnp.float32, smallest / len(pieces), high / len(pieces))
        loudness = loudness * jnp.repeat(jnp.exp(draws), shape[position] // parts).reshape((-1,) + (1,) * (len(shape) - 1 - position))
    return loudness


def rank_table(count, skew):
    loads = [(1 << 20) // math.isqrt(rank ** skew) + 1 for rank in range(1, count + 1)]
    width = 1 + sum(loads) // (1 << 30)
    return np.cumsum(np.array([max(1, weight // width) for weight in loads]))


def skewed_ids(stream_key, dims, number_of, lean):
    listing = rank_table(number_of, lean)
    lot = jax.random.randint(jax.random.fold_in(stream_key, 1), dims, 0, int(listing[number_of - 1]))
    rank = jnp.searchsorted(jnp.asarray(listing, jnp.int32), lot, side="right")
    return jax.random.permutation(jax.random.fold_in(stream_key, 2), number_of)[rank].astype(jnp.int32)


def assign_block(stream_key, own, number, rows, count, top, bound, lean):
    order = jax.random.permutation(stream_key, count)
    heavy_load, ordinary = portions_of(count, rows * top, bound, lean, True), portions_of(count, rows * top, bound, lean, False)
    places = jnp.arange(count)

    def named(tallies, rotation):
        used = int((tallies > 0).sum())
        fixed = max(1, used // 4)
        moved = fixed + (places - fixed + rotation * (used - fixed)) % max(1, count - fixed)
        return jnp.zeros((count,), jnp.int32).at[order[jnp.where(places < fixed, places, moved)]].set(jnp.asarray(tallies, jnp.int32))

    tallies = jnp.where(number % 4 == 0, named(heavy_load, number // 4), named(ordinary, number - number // 4 - 1))
    mixed = jax.random.permutation(jax.random.fold_in(own, 3), count)
    giver, sink = mixed[0:count // 2 * 2:2], mixed[1:count // 2 * 2:2]
    slack = jnp.minimum(tallies[giver] - 1, bound - tallies[sink]) // 2
    slack = jnp.where((giver == order[0]) | (sink == order[0]) | (tallies[sink] == 0), 0, jnp.maximum(slack, 0))
    moved = jax.random.randint(jax.random.fold_in(own, 4), (count // 2,), 0, 1 << 20) % (slack + 1)
    tallies = tallies.at[giver].add(-moved).at[sink].add(moved)
    labels = jnp.searchsorted(jnp.cumsum(tallies), jnp.arange(rows * top), side="right").astype(jnp.int32)
    table = labels.reshape(top, rows).T
    table = table[jax.random.permutation(jax.random.fold_in(own, 1), rows)]
    rotation = jax.random.randint(jax.random.fold_in(own, 2), (rows, 1), 0, top)
    return jnp.take_along_axis(table, (jnp.arange(top)[None, :] + rotation) % top, axis=1)


def portions_of(amount, total, reach, skew, full):
    portions = [(1 << 20) // math.isqrt(grade ** skew) + 1 for grade in range(1, amount + 1)]
    largest = reach if full else min(reach, max(-(-total // amount), total * portions[0] // sum(portions)))
    least = 1 if total - largest >= amount - 1 else 0
    given, rest = [largest] + [least] * (amount - 1), total - largest - least * (amount - 1)
    while rest > 0:
        movable = [i for i in range(1, amount) if given[i] < largest] or [i for i in range(1, amount) if given[i] < reach]
        mass, remaining = sum([portions[i] for i in movable]), rest
        for i in movable:
            extra = min(reach - given[i], max(1, remaining * portions[i] // mass), rest)
            given[i] = given[i] + extra
            rest = rest - extra
    return np.array(given)


def noise(own_key, shape, deviation, most, cuts=(), kind=jnp.bfloat16):
    factor_of = block_levels(own_key, shape, cuts, -0.22, 0.18) if cuts else 1.0
    entries = jax.random.normal(own_key, shape, jnp.float32) * deviation * factor_of
    return jnp.minimum(jnp.maximum(entries, -most), most).astype(kind)


def setup_inputs(seed: int = 0) -> dict:
    arg_keys = jax.random.split(jax.random.key(seed), 17)
    queries = draw_queries(jax.random.fold_in(arg_keys[16], 71), 0)
    cache_keys = draw_cache_keys(jax.random.fold_in(arg_keys[16], 71), 0)
    cache_values = noise(arg_keys[2], (PROMPTS, SAMPLES, CACHE, KVH * HD), 1.0, 6.0, ((0, 4), (1, 8)))
    new_keys = noise(arg_keys[3], (STEPS, PROMPTS, SAMPLES, KVH * HD), 1.5, 9.0, ((1, 4), (2, 8)))
    new_values = noise(arg_keys[4], (STEPS, PROMPTS, SAMPLES, KVH * HD), 1.0, 6.0, ((1, 4), (2, 8)))
    cache_len = draw_cache_len(jax.random.fold_in(arg_keys[16], 71), 0)
    o_proj = noise(arg_keys[6], (QH * HD, D), (QH * HD) ** -0.5, 0.125, ((1, 8),))
    residual_in = draw_residual_in(jax.random.fold_in(arg_keys[16], 71), 0)
    norm_gain = jnp.clip(1.0 + 0.18 * jax.random.normal(arg_keys[8], (D,), jnp.float32), 0.1, 1.9)
    router = noise(arg_keys[9], (D, E), D ** -0.5, 0.09375, ((0, 8),), jnp.float32)
    expert_gate = noise(arg_keys[10], (E * SPLIT, D, FFW // SPLIT), D ** -0.5, 0.09375, ((0, 8), (2, 4)))
    expert_up = noise(arg_keys[11], (E * SPLIT, D, FFW // SPLIT), D ** -0.5, 0.09375, ((0, 8), (2, 4)))
    expert_down = noise(arg_keys[12], (E * SPLIT, FFW // SPLIT, D), FFW ** -0.5, 0.046875, ((0, 8), (1, 4)))
    routes_keys = jax.random.split(jax.random.fold_in(arg_keys[13], 1), STEPS * PROMPTS * SAMPLES // (PROMPT_DEV * SAMPLES))
    routes_turns = jax.random.permutation(jax.random.fold_in(arg_keys[13], 3), STEPS * PROMPTS * SAMPLES // (PROMPT_DEV * SAMPLES))
    routes = jax.vmap(lambda own, number: assign_block(jax.random.fold_in(arg_keys[13], 2), own, number, PROMPT_DEV * SAMPLES, E, TOP, CAP, 1))(routes_keys, routes_turns).reshape((STEPS, PROMPTS, SAMPLES, TOP))
    answers = touch_ends(skewed_ids(arg_keys[14], (STEPS, PROMPTS, SAMPLES), ANSWERS, 2), jax.random.fold_in(arg_keys[14], 3), 0, ANSWERS - 1).astype(jnp.int32)
    stop_mask = touch_ends((jax.random.randint(arg_keys[15], (STEPS, PROMPTS), 0, 4) < 1).astype(jnp.int32), jax.random.fold_in(arg_keys[15], 1), 0, 1)
    return {"queries": queries, "cache_keys": cache_keys, "cache_values": cache_values, "new_keys": new_keys, "new_values": new_values, "cache_len": cache_len, "o_proj": o_proj, "residual_in": residual_in, "norm_gain": norm_gain, "router": router, "expert_gate": expert_gate, "expert_up": expert_up, "expert_down": expert_down, "routes": routes, "answers": answers, "stop_mask": stop_mask}


EPSILON = 1e-05

def attend(query, keys, values, fresh_keys, fresh_values, lengths):
    step_count = query.shape[0]
    row_count = query.shape[1]
    cache_size = keys.shape[1]
    group_size = QH // KVH
    score_scale = HD ** (-0.5)
    queried = query.astype(jnp.float32).reshape(step_count, row_count, KVH, group_size, HD)
    old_keys = keys.astype(jnp.float32).reshape(row_count, cache_size, KVH, HD)
    old_values = values.astype(jnp.float32).reshape(row_count, cache_size, KVH, HD)
    young_keys = fresh_keys.astype(jnp.float32).reshape(step_count, row_count, KVH, HD)
    young_values = fresh_values.astype(jnp.float32).reshape(step_count, row_count, KVH, HD)
    old_scores = jnp.einsum('trkgd,rckd->rkgtc', queried, old_keys) * score_scale
    new_scores = jnp.einsum('trkgd,urkd->rkgtu', queried, young_keys) * score_scale
    old_valid = jnp.arange(cache_size, dtype=jnp.int32)[None, :] < lengths[:, None]
    old_scores = jnp.where(old_valid[:, None, None, None, :], old_scores, -jnp.inf)
    new_valid = jnp.arange(step_count)[None, :] <= jnp.arange(step_count)[:, None]
    new_scores = jnp.where(new_valid, new_scores, -jnp.inf)
    highest = jnp.maximum(lax.optimization_barrier(jnp.max(old_scores, -1)), lax.optimization_barrier(jnp.max(new_scores, -1)))[..., None]
    old_exp = jnp.exp(old_scores - highest)
    new_exp = jnp.exp(new_scores - highest)
    denominator = lax.optimization_barrier(jnp.sum(old_exp, -1, keepdims=True)) + lax.optimization_barrier(jnp.sum(new_exp, -1, keepdims=True))
    old_weights = (old_exp / denominator).astype(jnp.bfloat16)
    new_weights = (new_exp / denominator).astype(jnp.bfloat16)
    combined = jnp.einsum('rkgtc,rckd->trkgd', old_weights.astype(jnp.float32), old_values)
    combined = combined + jnp.einsum('rkgtu,urkd->trkgd', new_weights.astype(jnp.float32), young_values)
    return combined.reshape(step_count, row_count, QH * HD).astype(jnp.bfloat16)

def per_prompt(operands):
    query, keys, values, fresh_keys, fresh_values, lengths = operands
    return attend(query, keys, values, fresh_keys, fresh_values, lengths)

def expert_pass(operands):
    tokens, w_gate, w_up, w_down = operands
    gate_part = jnp.dot(tokens, w_gate, preferred_element_type=jnp.float32)
    up_part = jnp.dot(tokens, w_up, preferred_element_type=jnp.float32)
    hidden = (jax.nn.silu(gate_part) * up_part).astype(jnp.bfloat16)
    return jnp.dot(hidden, w_down, preferred_element_type=jnp.float32)

def reference(queries, cache_keys, cache_values, new_keys, new_values, cache_len, o_proj, residual_in, norm_gain, router, expert_gate, expert_up, expert_down, routes, answers, stop_mask):
    attended = lax.map(per_prompt, (jnp.moveaxis(queries, 1, 0), cache_keys, cache_values, jnp.moveaxis(new_keys, 1, 0), jnp.moveaxis(new_values, 1, 0), cache_len))
    attended = jnp.moveaxis(attended, 0, 1)
    row_total = STEPS * PROMPTS * SAMPLES
    attn_proj = jnp.dot(attended.reshape(row_total, QH * HD), o_proj, preferred_element_type=jnp.float32)
    mixed_rows = residual_in.reshape(row_total, D).astype(jnp.float32) + attn_proj
    inv_rms = lax.rsqrt(lax.optimization_barrier(jnp.mean(mixed_rows * mixed_rows, -1, keepdims=True)) + EPSILON)
    normed_f = mixed_rows * inv_rms * norm_gain
    normed = normed_f.astype(jnp.bfloat16)
    logits = jnp.dot(normed_f, router, precision=lax.Precision.HIGHEST)
    picks = routes.reshape(row_total, TOP)
    chosen = jnp.take_along_axis(logits, picks, axis=1)
    gate_weights = jax.nn.sigmoid(chosen - chosen[:, ::-1])
    block_rows = PROMPT_DEV * SAMPLES
    block_count = row_total // block_rows
    expert_hot = (picks[:, :, None] == jnp.arange(E, dtype=jnp.int32)).astype(jnp.int32)
    flat_hot = expert_hot.reshape(block_count, block_rows * TOP, E)
    earlier = jnp.cumsum(flat_hot, axis=1) - flat_hot
    place = lax.optimization_barrier(jnp.sum(earlier * flat_hot, -1)).reshape(row_total, TOP)
    block_of = (jnp.arange(row_total, dtype=jnp.int32) // block_rows)[:, None]
    slot_ids = (picks * block_count + block_of) * CAP + place
    slot_total = E * block_count * CAP
    owners = jnp.zeros((slot_total,), jnp.int32).at[slot_ids.reshape(-1)].set(jnp.arange(row_total * TOP, dtype=jnp.int32) // TOP + 1)
    padded = jnp.concatenate([jnp.zeros((1, D), jnp.bfloat16), normed], 0)
    slot_rows = padded[owners].reshape(E, block_count * CAP, D)
    full_gate = expert_gate.reshape(E, SPLIT, D, FFW // SPLIT).transpose(0, 2, 1, 3).reshape(E, D, FFW)
    full_up = expert_up.reshape(E, SPLIT, D, FFW // SPLIT).transpose(0, 2, 1, 3).reshape(E, D, FFW)
    full_down = expert_down.reshape(E, FFW, D)
    expert_out = lax.map(expert_pass, (slot_rows, full_gate, full_up, full_down)).reshape(slot_total, D)
    picked = expert_out[slot_ids.reshape(-1)].reshape(row_total, TOP, D)
    moe = lax.optimization_barrier(jnp.sum(gate_weights[:, :, None] * picked, 1))
    active = (1 - stop_mask).astype(jnp.float32)
    active_rows = jnp.broadcast_to(active[:, :, None], (STEPS, PROMPTS, SAMPLES)).reshape(row_total, 1)
    updated = residual_in.reshape(row_total, D).astype(jnp.float32) + active_rows * (attn_proj + moe)
    residual_out = updated.reshape(STEPS, PROMPTS, SAMPLES, D).astype(jnp.bfloat16)
    hits = lax.optimization_barrier(jnp.sum((answers[..., None] == jnp.arange(ANSWERS, dtype=jnp.int32)).astype(jnp.float32), 2))
    votes = active[:, :, None] * hits
    tally = jnp.cumsum(votes, 0)
    vote_share = tally / jnp.maximum(lax.optimization_barrier(jnp.sum(tally, -1, keepdims=True)), 1.0)
    return (residual_out, vote_share)
```

```python
import jax
import jax.numpy as jnp
from jax import lax
from jax.experimental import pallas as pl
from jax.experimental.pallas import tpu as pltpu
from jax.sharding import PartitionSpec as P

E = 8
TOP = 2
HD = 128
ANSWERS = 128
EPSILON = 1e-05
LANES = 128
BF = jnp.bfloat16
F32 = jnp.float32

VM = pl.BlockSpec(memory_space=pltpu.VMEM)
SM = pl.BlockSpec(memory_space=pltpu.SMEM)
AN = pl.BlockSpec(memory_space=pl.ANY)


def held(x):
    return pltpu.with_memory_space_constraint(x, pltpu.VMEM)


def parked(x):
    return pltpu.with_memory_space_constraint(x, pltpu.HBM)


def contract(a, b, ca, cb):
    return lax.dot_general(a, b, (((ca,), (cb,)), ((), ())), preferred_element_type=F32)


def mebi(size):
    return size >> 20


def params(flops, mib):
    return dict(
        compiler_params=pltpu.CompilerParams(vmem_limit_bytes=mib << 20),
        cost_estimate=pl.CostEstimate(flops=flops, transcendentals=0, bytes_accessed=1 << 20),
    )


def attention(queries, keys, values, new_keys, new_values, lengths, answers, routes, peers, capacity, samples):
    _, _, steps, width = queries.shape
    table_rows = steps * samples
    slot_count = steps * capacity
    cache, kv_width = keys.shape[2:]
    kv_heads, heads = kv_width // HD, width // HD
    group = heads // kv_heads
    tail = cache - 16

    def body(q_ref, k_hbm, v_hbm, nk_ref, nv_ref, len_ref, ans_ref, routes_ref, out_ref, place_ref, expert_ref, k_s, v_s, q_s, o_s, used, sems):
        ck = pltpu.make_async_copy(k_hbm.at[0, 0], k_s, sems.at[0])
        cv = pltpu.make_async_copy(v_hbm.at[0, 0], v_s, sems.at[1])
        ck.start()
        cv.start()
        for t in range(steps):
            q = q_ref[0, 0, t : t + 1, :].astype(F32)
            for h in range(heads):
                k, g = divmod(h, group)
                q_s[pl.ds((k * group + g) * steps + t, 1), :] = q[:, h * HD : (h + 1) * HD]
        prompt = lax.axis_index("dp")
        slot_lane = lax.broadcasted_iota(jnp.int32, (1, E * slot_count), 1)
        expert_lane = lax.broadcasted_iota(jnp.int32, (1, LANES), 1)
        for i in range(steps * E):
            used[i] = 0
        for t in range(steps):

            def one(s, _):
                for k in range(TOP):
                    e = routes_ref[t, prompt, k, s]
                    place = used[t * E + e]
                    used[t * E + e] = place + 1
                    slot = e * slot_count + t * capacity + place
                    n = k * table_rows + t * samples + s
                    place_ref[pl.ds(n, 1), :] = (slot_lane == slot).astype(F32)
                    expert_ref[pl.ds(n, 1), :] = (expert_lane == e).astype(F32)
                return 0

            lax.fori_loop(0, samples, one, 0)
        length = len_ref[0, 0]
        rows = group * steps
        position = lax.broadcasted_iota(jnp.int32, (rows, cache), 1)
        step = lax.broadcasted_iota(jnp.int32, (rows, cache), 0) % steps
        fresh = position - (cache - steps)
        valid = (position < length) | ((fresh >= 0) & (fresh <= step))
        row = lax.broadcasted_iota(jnp.int32, (16, kv_width), 0)

        def refresh(s_ref, new_ref):
            last = s_ref[tail:, :].astype(F32)
            for u in range(steps):
                last = jnp.where(row == 16 - steps + u, new_ref[0, 0, u : u + 1, :].astype(F32), last)
            s_ref[tail:, :] = last.astype(BF)

        ck.wait()
        refresh(k_s, nk_ref)
        weights = []
        for k in range(kv_heads):
            q = q_s[k * rows : (k + 1) * rows, :].astype(BF)
            scores = contract(q, k_s[:, k * HD : (k + 1) * HD], 1, 1) * (HD**-0.5)
            scores = jnp.where(valid, scores, -jnp.inf)
            e = jnp.exp(scores - jnp.max(scores, -1, keepdims=True))
            weights.append((e / jnp.sum(e, -1, keepdims=True)).astype(BF))
        cv.wait()
        refresh(v_s, nv_ref)
        for k in range(kv_heads):
            o = contract(weights[k], v_s[:, k * HD : (k + 1) * HD], 1, 0)
            for g in range(group):
                h = k * group + g
                o_s[:, h * HD : (h + 1) * HD] = o[g * steps : (g + 1) * steps, :]
        lane = lax.broadcasted_iota(jnp.int32, (1, ANSWERS), 1)
        for t in range(steps):
            o_s[t : t + 1, width:] = (lane == ans_ref[0, 0, t]).astype(F32)
        payload = o_s[...].astype(BF)
        for i in range(peers):
            out_ref[i] = payload

    return pl.pallas_call(
        body,
        in_specs=[VM, AN, AN, VM, VM, SM, SM, SM],
        out_specs=[VM] * 3,
        out_shape=[
            jax.ShapeDtypeStruct((peers, steps, width + ANSWERS), BF),
            jax.ShapeDtypeStruct((TOP * table_rows, E * slot_count), F32),
            jax.ShapeDtypeStruct((TOP * table_rows, LANES), F32),
        ],
        scratch_shapes=[
            pltpu.VMEM((cache, kv_width), BF),
            pltpu.VMEM((cache, kv_width), BF),
            pltpu.VMEM((heads * steps, HD), F32),
            pltpu.VMEM((steps, width + ANSWERS), F32),
            pltpu.SMEM((steps * E,), jnp.int32),
            pltpu.SemaphoreType.DMA((2,)),
        ],
        name="attention",
        **params(1 << 36, 3),
    )(queries, parked(keys), parked(values), new_keys, new_values, lengths, answers, routes)


def projection(recv, o_proj, residual, gain, router, places, experts, stops, groups, spread):
    peers, steps, wide = recv.shape
    width = wide - ANSWERS
    columns = o_proj.shape[1]
    samples = residual.shape[2]
    rows = steps * samples
    slots = places.shape[1]
    slot_count = slots // E
    payload = columns + LANES

    def body(
        recv_ref, o_ref, res_ref, gain_ref, router_ref, place_ref, expert_ref, stop_ref, out_ref, attn_ref, vote_ref
    ):
        x = jnp.concatenate([recv_ref[i] for i in range(peers)], 0)
        to = lax.broadcasted_iota(jnp.int32, (rows, rows), 0)
        at = lax.broadcasted_iota(jnp.int32, (rows, rows), 1)
        order = (at == (to % samples) * steps + to // samples).astype(BF)
        x = contract(order, x, 1, 0)
        tally = jnp.zeros((1, ANSWERS), F32)
        for t in range(steps):
            hits = jnp.sum(x[t * samples : (t + 1) * samples, width:], 0, keepdims=True)
            tally = tally + (1 - stop_ref[0, t]).astype(F32) * hits
            vote_ref[t] = tally / jnp.maximum(jnp.sum(tally, -1, keepdims=True), 1.0)
        attn = contract(x[:, :width].astype(BF), o_ref[...], 1, 0)
        attn_ref[...] = attn
        residual = jnp.concatenate([res_ref[t, 0].astype(F32) for t in range(steps)], 0)
        mixed = residual + attn
        squares = jnp.sum(mixed * mixed, -1, keepdims=True)
        scaled = mixed * gain_ref[...]
        logits = lax.dot_general(
            scaled,
            router_ref[...],
            (((1,), (1,)), ((), ())),
            precision=lax.Precision.HIGHEST,
            preferred_element_type=F32,
        )
        hot = expert_ref[:, :E]
        difference = jnp.sum(logits * (hot[:rows] - hot[rows:]), -1, keepdims=True)
        lane = lax.broadcasted_iota(jnp.int32, (rows, LANES), 1)
        stacked = []
        for sign in (1.0, -1.0):
            stats = jnp.where(lane == 0, squares, jnp.where(lane == 1, sign * difference, 0.0))
            high = stats.astype(BF).astype(F32)
            rest = stats - high
            middle = rest.astype(BF).astype(F32)
            low = rest - middle
            stats = high + pltpu.roll(middle, 2, 1) + pltpu.roll(low, 4, 1)
            stacked.append(jnp.concatenate([scaled.astype(BF), stats.astype(BF)], 1))
        by_slot = contract(place_ref[...].astype(BF), jnp.concatenate(stacked, 0), 0, 0).astype(BF)
        for e in range(E):
            block = by_slot[e * slot_count : (e + 1) * slot_count, :]
            for group in range(groups):
                for copy in range(spread):
                    out_ref[group * E * spread + e * spread + copy] = block

    return pl.pallas_call(
        body,
        in_specs=[VM] * 7 + [SM],
        out_specs=[VM] * 3,
        out_shape=[
            jax.ShapeDtypeStruct((groups * peers, slot_count, payload), BF),
            jax.ShapeDtypeStruct((rows, columns), F32),
            jax.ShapeDtypeStruct((steps, 1, ANSWERS), F32),
        ],
        name="projection",
        **params(1 << 36, 3 + mebi(2 * groups * peers * slot_count * payload * 2)),
    )(recv, held(o_proj), held(residual), held(gain), held(router), places, experts, stops)


def expert(recv, gate, up, down, peers, columns):
    groups = recv.shape[0] // peers
    slot_count = recv.shape[1]
    tokens = groups * slot_count
    width, hidden = gate.shape
    block = 512 if hidden % 512 == 0 else hidden
    piece = 256 if block % 256 == 0 else block
    pieces = block // piece
    slots = 2

    def body(recv_ref, g_ref, u_ref, down_hbm, out_ref, x_s, d_s, acc_s, sems):
        def fetch(n):
            at = pl.ds(pl.multiple_of(n * piece, 64), piece)
            return pltpu.make_async_copy(down_hbm.at[0, at, :], d_s.at[n % slots], sems.at[n % slots])

        for n in range(min(slots, hidden // piece)):
            fetch(n).start()
        inverse, weight = [], []
        for i in range(groups):
            total = recv_ref[i * peers, :, columns:].astype(F32)
            for c in range(1, peers):
                total = total + recv_ref[i * peers + c, :, columns:].astype(F32)
            total = total + pltpu.roll(total, LANES - 2, 1) + pltpu.roll(total, LANES - 4, 1)
            inv = lax.rsqrt(total[:, 0:1] / width + EPSILON)
            inverse.append(inv)
            weight.append(1.0 / (1.0 + jnp.exp(-inv * total[:, 1:2])))
        inverse = jnp.concatenate(inverse, 0)
        weight = jnp.concatenate(weight, 0)
        for c in range(peers):
            x_s[:, c * columns : (c + 1) * columns] = jnp.concatenate(
                [recv_ref[i * peers + c, :, :columns] for i in range(groups)], 0
            )
        acc_s[...] = jnp.zeros_like(acc_s)

        def step(i, _):
            at = pl.ds(pl.multiple_of(i * block, LANES if block % LANES == 0 else 1), block)
            g = contract(x_s[...], g_ref[:, at], 1, 0) * inverse
            u = contract(x_s[...], u_ref[:, at], 1, 0) * inverse
            h = (g / (1.0 + jnp.exp(-g)) * u).astype(BF)
            for k in range(pieces):
                n = i * pieces + k
                fetch(n).wait()
                acc_s[...] += contract(h[:, k * piece : (k + 1) * piece], d_s[n % slots], 1, 0)

                @pl.when(n + slots < hidden // piece)
                def _():
                    fetch(n + slots).start()

            return 0

        lax.fori_loop(0, hidden // block, step, 0)
        for c in range(peers):
            mine = (acc_s[:, c * columns : (c + 1) * columns] * weight).astype(BF)
            for i in range(groups):
                out_ref[i * peers + c] = mine[i * slot_count : (i + 1) * slot_count, :]

    return pl.pallas_call(
        body,
        in_specs=[VM, VM, VM, AN],
        out_specs=VM,
        out_shape=jax.ShapeDtypeStruct((groups * peers, slot_count, columns), BF),
        scratch_shapes=[
            pltpu.VMEM((tokens, width), BF),
            pltpu.VMEM((slots, piece, width), BF),
            pltpu.VMEM((tokens, width), F32),
            pltpu.SemaphoreType.DMA((slots,)),
        ],
        name="expert",
        **params(1 << 33, 4 + 2 * mebi(recv.size * 2 + tokens * width * 6)),
    )(recv, held(gate), held(up), parked(down))


def combine(recv, places, attn, residual, stops, groups, spread):
    steps, _, samples, columns = residual.shape
    rows = steps * samples
    peers = E * spread

    def body(recv_ref, place_ref, attn_ref, res_ref, stop_ref, out_ref):
        pick = place_ref[:rows, :]
        for k in range(1, TOP):
            pick = pick + place_ref[k * rows : (k + 1) * rows, :]
        pick = pick.astype(BF)
        moe = jnp.zeros((rows, columns), F32)
        for group in range(groups):
            for copy in range(spread):
                mine = jnp.concatenate([recv_ref[group * peers + e * spread + copy] for e in range(E)], 0)
                moe = moe + contract_rows(pick, mine)
        update = attn_ref[...] + moe
        for t in range(steps):
            active = (1 - stop_ref[0, t]).astype(F32)
            fresh = res_ref[t, 0].astype(F32) + active * update[t * samples : (t + 1) * samples, :]
            out_ref[t, 0] = fresh.astype(BF)

    def contract_rows(pick, mine):
        return contract(pick, mine, 1, 0)

    return pl.pallas_call(
        body,
        in_specs=[VM] * 4 + [SM],
        out_specs=VM,
        out_shape=jax.ShapeDtypeStruct(residual.shape, BF),
        name="combine",
        **params(1 << 26, 3 + mebi(2 * recv.size * 2)),
    )(recv, places, attn, held(residual), stops)


def on_device(
    queries,
    cache_keys,
    cache_values,
    new_keys,
    new_values,
    cache_len,
    o_proj,
    residual_in,
    norm_gain,
    router,
    expert_gate,
    expert_up,
    expert_down,
    routes,
    answers,
    stop_mask,
):
    peers = lax.axis_size("expert")
    groups = lax.axis_size("dp")
    spread = peers // E
    samples, columns = residual_in.shape[2:]
    capacity = 2 * residual_in.shape[1] * samples * TOP // E
    gate, up = expert_gate.reshape(expert_gate.shape[1:]), expert_up.reshape(expert_up.shape[1:])
    stops = stop_mask.T
    payload, places, experts = attention(
        jnp.transpose(queries, (1, 2, 0, 3)),
        cache_keys,
        cache_values,
        jnp.transpose(new_keys, (1, 2, 0, 3)),
        jnp.transpose(new_values, (1, 2, 0, 3)),
        cache_len,
        jnp.transpose(answers, (1, 2, 0)),
        jnp.transpose(routes, (0, 1, 3, 2)),
        peers,
        capacity,
        samples,
    )
    recv = lax.all_to_all(payload, "expert", split_axis=0, concat_axis=0, tiled=True)
    outgoing, attn, votes = projection(
        recv, o_proj, residual_in, norm_gain.reshape(1, columns), router.T, places, experts, stops, groups, spread
    )
    tokens = lax.all_to_all(outgoing, ("dp", "expert"), split_axis=0, concat_axis=0, tiled=True)
    partial = expert(tokens, gate, up, expert_down, peers, columns)
    returned = lax.all_to_all(partial, ("dp", "expert"), split_axis=0, concat_axis=0, tiled=True)
    updated = combine(returned, places, attn, residual_in, stops, groups, spread)
    return updated, votes


def solution(mesh):
    placed = (
        P(None, "dp", "expert", None),
        P("dp", "expert", None, None),
        P("dp", "expert", None, None),
        P(None, "dp", "expert", None),
        P(None, "dp", "expert", None),
        P("dp", "expert"),
        P(None, "expert"),
        P(None, "dp", None, "expert"),
        P("expert"),
        P("expert", None),
        P("expert", None, "dp"),
        P("expert", None, "dp"),
        P("expert", "dp", None),
        P(),
        P(None, "dp", "expert"),
        P(None, "dp"),
    )
    return jax.shard_map(
        on_device,
        mesh=mesh,
        in_specs=placed,
        out_specs=(P(None, "dp", None, "expert"), P(None, "dp", None)),
        check_vma=False,
    )
```

```python
import jax
import jax.numpy as jnp
from jax import lax
from jax.experimental import pallas as pl
from jax.experimental.pallas import tpu as pltpu
from jax.sharding import PartitionSpec as P

E = 8
TOP = 2
HD = 128
ANSWERS = 128
EPSILON = 1e-05
LANES = 128
BF = jnp.bfloat16
F32 = jnp.float32

VM = pl.BlockSpec(memory_space=pltpu.VMEM)
SM = pl.BlockSpec(memory_space=pltpu.SMEM)
AN = pl.BlockSpec(memory_space=pl.ANY)


def held(x):
    return pltpu.with_memory_space_constraint(x, pltpu.VMEM)


def parked(x):
    return pltpu.with_memory_space_constraint(x, pltpu.HBM)


def contract(a, b, ca, cb):
    return lax.dot_general(a, b, (((ca,), (cb,)), ((), ())), preferred_element_type=F32)


def mebi(size):
    return size >> 20


def params(flops, mib):
    return dict(
        compiler_params=pltpu.CompilerParams(vmem_limit_bytes=int(mib * (1 << 20))),
        cost_estimate=pl.CostEstimate(flops=flops, transcendentals=0, bytes_accessed=1 << 20),
    )


def attention(queries, keys, values, new_keys, new_values, lengths, answers, routes, o_proj, peers, capacity, samples):
    _, _, steps, width = queries.shape
    table_rows = steps * samples
    slot_count = steps * capacity
    cache, kv_width = keys.shape[2:]
    kv_heads, heads = kv_width // HD, width // HD
    group = heads // kv_heads
    rows = group * steps
    first = cache - steps

    def body(
        q_ref,
        k_ref,
        v_ref,
        nk_ref,
        nv_ref,
        len_ref,
        ans_ref,
        routes_ref,
        o_hbm,
        out_ref,
        place_ref,
        expert_ref,
        o_ref,
        q_s,
        a_s,
        used,
        sem,
    ):
        move = pltpu.make_async_copy(o_hbm, o_ref, sem)
        move.start()
        prompt = lax.axis_index("dp")
        slot_lane = lax.broadcasted_iota(jnp.int32, (1, E * slot_count), 1)
        expert_lane = lax.broadcasted_iota(jnp.int32, (1, LANES), 1)
        for i in range(steps * E):
            used[i] = 0
        for t in range(steps):

            def one(s, _):
                for k in range(TOP):
                    e = routes_ref[t, prompt, k, s]
                    place = used[t * E + e]
                    used[t * E + e] = place + 1
                    slot = e * slot_count + t * capacity + place
                    n = k * table_rows + t * samples + s
                    place_ref[pl.ds(n, 1), :] = (slot_lane == slot).astype(F32)
                    expert_ref[pl.ds(n, 1), :] = (expert_lane == e).astype(F32)
                return 0

            lax.fori_loop(0, samples, one, 0)
        for t in range(steps):
            q = q_ref[0, 0, t : t + 1, :].astype(F32)
            for h in range(heads):
                q_s[pl.ds(h * steps + t, 1), :] = q[:, h * HD : (h + 1) * HD]
        position = lax.broadcasted_iota(jnp.int32, (rows, cache), 1)
        step = lax.broadcasted_iota(jnp.int32, (rows, cache), 0) % steps
        fresh = position - first
        valid = (position < len_ref[0, 0]) | ((fresh >= 0) & (fresh <= step))
        new_keys = nk_ref[0, 0].astype(F32)
        new_values = nv_ref[0, 0].astype(F32)
        for k in range(kv_heads):
            at = slice(k * HD, (k + 1) * HD)
            q = q_s[k * rows : (k + 1) * rows, :]
            scores = contract(q.astype(BF), k_ref[0, 0, :, at], 1, 1)
            for u in range(steps):
                score = jnp.sum(q * new_keys[u : u + 1, at], -1, keepdims=True)
                scores = jnp.where(fresh == u, score, scores)
            scores = jnp.where(valid, scores * (HD**-0.5), -jnp.inf)
            e = jnp.exp(scores - jnp.max(scores, -1, keepdims=True))
            weights = (e / jnp.sum(e, -1, keepdims=True)).astype(BF)
            o = contract(jnp.where(fresh < 0, weights, jnp.zeros_like(weights)), v_ref[0, 0, :, at], 1, 0)
            weights = weights.astype(F32)
            for u in range(steps):
                weight = jnp.sum(jnp.where(fresh == u, weights, 0.0), -1, keepdims=True)
                o = o + weight * new_values[u : u + 1, at]
            for g in range(group):
                h = k * group + g
                a_s[:, h * HD : (h + 1) * HD] = o[g * steps : (g + 1) * steps, :]
        lane = lax.broadcasted_iota(jnp.int32, (1, ANSWERS), 1)
        for t in range(steps):
            a_s[t : t + 1, width:] = (lane == ans_ref[0, 0, t]).astype(F32)
        payload = a_s[...].astype(BF)
        for i in range(peers):
            out_ref[i] = payload
        move.wait()

    return pl.pallas_call(
        body,
        in_specs=[VM, VM, VM, VM, VM, SM, SM, SM, AN],
        out_specs=[VM] * 4,
        out_shape=[
            jax.ShapeDtypeStruct((peers, steps, width + ANSWERS), BF),
            jax.ShapeDtypeStruct((TOP * table_rows, E * slot_count), F32),
            jax.ShapeDtypeStruct((TOP * table_rows, LANES), F32),
            pltpu.VMEM(o_proj.shape, o_proj.dtype),
        ],
        scratch_shapes=[
            pltpu.VMEM((heads * steps, HD), F32),
            pltpu.VMEM((steps, width + ANSWERS), F32),
            pltpu.SMEM((steps * E,), jnp.int32),
            pltpu.SemaphoreType.DMA,
        ],
        name="attention",
        **params(1 << 36, 2),
    )(
        *[parked(x) for x in (queries, keys, values, new_keys, new_values)],
        lengths,
        *[parked(x) for x in (answers, routes, o_proj)],
    )


def projection(recv, o_proj, residual, gain, router, places, experts, stops, groups, spread):
    peers, steps, wide = recv.shape
    width = wide - ANSWERS
    columns = o_proj.shape[1]
    samples = residual.shape[2]
    rows = steps * samples
    slots = places.shape[1]
    slot_count = slots // E
    payload = columns + LANES

    def body(
        recv_ref, o_ref, res_ref, gain_ref, router_ref, place_ref, expert_ref, stop_ref, out_ref, attn_ref, vote_ref
    ):
        x = jnp.concatenate([recv_ref[i] for i in range(peers)], 0)
        to = lax.broadcasted_iota(jnp.int32, (rows, rows), 0)
        at = lax.broadcasted_iota(jnp.int32, (rows, rows), 1)
        order = (at == (to % samples) * steps + to // samples).astype(BF)
        x = contract(order, x, 1, 0)
        tally = jnp.zeros((1, ANSWERS), F32)
        for t in range(steps):
            hits = jnp.sum(x[t * samples : (t + 1) * samples, width:], 0, keepdims=True)
            tally = tally + (1 - stop_ref[0, t]).astype(F32) * hits
            vote_ref[t] = tally / jnp.maximum(jnp.sum(tally, -1, keepdims=True), 1.0)
        attn = contract(x[:, :width].astype(BF), o_ref[...], 1, 0)
        attn_ref[...] = attn
        residual = jnp.concatenate([res_ref[t, 0].astype(F32) for t in range(steps)], 0)
        mixed = residual + attn
        squares = jnp.sum(mixed * mixed, -1, keepdims=True)
        scaled = mixed * gain_ref[...]
        logits = lax.dot_general(
            scaled,
            router_ref[...],
            (((1,), (1,)), ((), ())),
            precision=lax.Precision.HIGHEST,
            preferred_element_type=F32,
        )
        hot = expert_ref[:, :E]
        difference = jnp.sum(logits * (hot[:rows] - hot[rows:]), -1, keepdims=True)
        lane = lax.broadcasted_iota(jnp.int32, (rows, LANES), 1)
        stacked = []
        for sign in (1.0, -1.0):
            stats = jnp.where(lane == 0, squares, jnp.where(lane == 1, sign * difference, 0.0))
            high = stats.astype(BF).astype(F32)
            rest = stats - high
            middle = rest.astype(BF).astype(F32)
            low = rest - middle
            stats = high + pltpu.roll(middle, 2, 1) + pltpu.roll(low, 4, 1)
            stacked.append(jnp.concatenate([scaled.astype(BF), stats.astype(BF)], 1))
        by_slot = contract(place_ref[...].astype(BF), jnp.concatenate(stacked, 0), 0, 0).astype(BF)
        for e in range(E):
            block = by_slot[e * slot_count : (e + 1) * slot_count, :]
            for group in range(groups):
                for copy in range(spread):
                    out_ref[group * E * spread + e * spread + copy] = block

    return pl.pallas_call(
        body,
        in_specs=[VM] * 7 + [SM],
        out_specs=[VM] * 3,
        out_shape=[
            jax.ShapeDtypeStruct((groups * peers, slot_count, payload), BF),
            jax.ShapeDtypeStruct((rows, columns), F32),
            jax.ShapeDtypeStruct((steps, 1, ANSWERS), F32),
        ],
        name="projection",
        **params(1 << 36, 2 + mebi(2 * groups * peers * slot_count * payload * 2)),
    )(recv, held(o_proj), held(residual), held(gain), held(router), places, experts, stops)


def expert(recv, gate, up, down, peers, columns):
    groups = recv.shape[0] // peers
    slot_count = recv.shape[1]
    tokens = groups * slot_count
    width, hidden = gate.shape
    block = 512 if hidden % 512 == 0 else hidden
    blocks = hidden // block
    piece = 128 if block % 128 == 0 else block
    pieces = hidden // piece
    slots = min(5, pieces)

    def body(recv_ref, g_ref, u_ref, down_hbm, out_ref, x_s, d_s, acc_s, sems):
        def fetch(n):
            at = pl.ds(n * piece, piece)
            return pltpu.make_async_copy(down_hbm.at[0, at, :], d_s.at[n % slots], sems.at[n % slots])

        for n in range(slots):
            fetch(n).start()
        inverse, weight = [], []
        for i in range(groups):
            total = recv_ref[i * peers, :, columns:].astype(F32)
            for c in range(1, peers):
                total = total + recv_ref[i * peers + c, :, columns:].astype(F32)
            total = total + pltpu.roll(total, LANES - 2, 1) + pltpu.roll(total, LANES - 4, 1)
            inv = lax.rsqrt(total[:, 0:1] / width + EPSILON)
            inverse.append(inv)
            weight.append(1.0 / (1.0 + jnp.exp(-inv * total[:, 1:2])))
        inverse = jnp.concatenate(inverse, 0)
        weight = jnp.concatenate(weight, 0)
        for c in range(peers):
            x_s[:, c * columns : (c + 1) * columns] = jnp.concatenate(
                [recv_ref[i * peers + c, :, :columns] for i in range(groups)], 0
            )
        def hidden_of(i):
            at = slice(i * block, (i + 1) * block)
            g = contract(x_s[...], g_ref[:, at], 1, 0) * inverse
            u = contract(x_s[...], u_ref[:, at], 1, 0) * inverse
            return (g / (1.0 + jnp.exp(-g)) * u).astype(BF)

        state = hidden_of(0)
        for i in range(1, blocks + 1):
            after = hidden_of(i) if i < blocks else None
            for n in range((i - 1) * block // piece, i * block // piece):
                fetch(n).wait()
                at = n * piece - (i - 1) * block
                out = contract(state[:, at : at + piece], d_s[n % slots], 1, 0)
                acc_s[...] = out if n == 0 else acc_s[...] + out
                if n + slots < pieces:
                    fetch(n + slots).start()
            state = after
        for c in range(peers):
            mine = (acc_s[:, c * columns : (c + 1) * columns] * weight).astype(BF)
            for i in range(groups):
                out_ref[i * peers + c] = mine[i * slot_count : (i + 1) * slot_count, :]

    return pl.pallas_call(
        body,
        in_specs=[VM, VM, VM, AN],
        out_specs=VM,
        out_shape=pltpu.VMEM((groups * peers, slot_count, columns), BF),
        scratch_shapes=[
            pltpu.VMEM((tokens, width), BF),
            pltpu.VMEM((slots, piece, width), BF),
            pltpu.VMEM((tokens, width), F32),
            pltpu.SemaphoreType.DMA((slots,)),
        ],
        name="expert",
        **params(1 << 33, 4.5 + 2 * mebi(recv.size * 2 + tokens * width * 6)),
    )(held(recv), held(gate), held(up), parked(down))


def combine(recv, places, attn, residual, stops, groups, spread):
    steps, _, samples, columns = residual.shape
    rows = steps * samples
    peers = E * spread

    def body(recv_ref, place_ref, attn_ref, res_ref, stop_ref, out_ref):
        pick = place_ref[:rows, :]
        for k in range(1, TOP):
            pick = pick + place_ref[k * rows : (k + 1) * rows, :]
        pick = pick.astype(BF)
        moe = jnp.zeros((rows, columns), F32)
        for group in range(groups):
            for copy in range(spread):
                mine = jnp.concatenate([recv_ref[group * peers + e * spread + copy] for e in range(E)], 0)
                moe = moe + contract_rows(pick, mine)
        update = attn_ref[...] + moe
        for t in range(steps):
            active = (1 - stop_ref[0, t]).astype(F32)
            fresh = res_ref[t, 0].astype(F32) + active * update[t * samples : (t + 1) * samples, :]
            out_ref[t, 0] = fresh.astype(BF)

    def contract_rows(pick, mine):
        return contract(pick, mine, 1, 0)

    return pl.pallas_call(
        body,
        in_specs=[VM] * 4 + [SM],
        out_specs=VM,
        out_shape=jax.ShapeDtypeStruct(residual.shape, BF),
        name="combine",
        **params(1 << 26, 3 + mebi(2 * recv.size * 2)),
    )(recv, places, attn, held(residual), stops)


def on_device(
    queries,
    cache_keys,
    cache_values,
    new_keys,
    new_values,
    cache_len,
    o_proj,
    residual_in,
    norm_gain,
    router,
    expert_gate,
    expert_up,
    expert_down,
    routes,
    answers,
    stop_mask,
):
    peers = lax.axis_size("expert")
    groups = lax.axis_size("dp")
    spread = peers // E
    samples, columns = residual_in.shape[2:]
    capacity = 2 * residual_in.shape[1] * samples * TOP // E
    gate, up = expert_gate.reshape(expert_gate.shape[1:]), expert_up.reshape(expert_up.shape[1:])
    stops = stop_mask.T
    payload, places, experts, o_v = attention(
        jnp.transpose(queries, (1, 2, 0, 3)),
        cache_keys,
        cache_values,
        jnp.transpose(new_keys, (1, 2, 0, 3)),
        jnp.transpose(new_values, (1, 2, 0, 3)),
        cache_len,
        jnp.transpose(answers, (1, 2, 0)),
        jnp.transpose(routes, (0, 1, 3, 2)),
        o_proj,
        peers,
        capacity,
        samples,
    )
    recv = lax.all_to_all(payload, "expert", split_axis=0, concat_axis=0, tiled=True)
    outgoing, attn, votes = projection(
        recv, o_v, residual_in, norm_gain.reshape(1, columns), router.T, places, experts, stops, groups, spread
    )
    tokens = lax.all_to_all(outgoing, ("dp", "expert"), split_axis=0, concat_axis=0, tiled=True)
    partial = expert(tokens, gate, up, expert_down, peers, columns)
    returned = lax.all_to_all(partial, ("dp", "expert"), split_axis=0, concat_axis=0, tiled=True)
    updated = combine(returned, places, attn, residual_in, stops, groups, spread)
    return updated, votes


def solution(mesh):
    placed = (
        P(None, "dp", "expert", None),
        P("dp", "expert", None, None),
        P("dp", "expert", None, None),
        P(None, "dp", "expert", None),
        P(None, "dp", "expert", None),
        P("dp", "expert"),
        P(None, "expert"),
        P(None, "dp", None, "expert"),
        P("expert"),
        P("expert", None),
        P("expert", None, "dp"),
        P("expert", None, "dp"),
        P("expert", "dp", None),
        P(),
        P(None, "dp", "expert"),
        P(None, "dp"),
    )
    return jax.shard_map(
        on_device,
        mesh=mesh,
        in_specs=placed,
        out_specs=(P(None, "dp", None, "expert"), P(None, "dp", None)),
        check_vma=False,
    )
```

```python
import jax
import jax.numpy as jnp
from jax import lax
from jax.experimental import pallas as pl
from jax.experimental.pallas import tpu as pltpu
from jax.sharding import PartitionSpec as P

E = 8
TOP = 2
HD = 128
ANSWERS = 128
EPSILON = 1e-05
LANES = 128
BF = jnp.bfloat16
F32 = jnp.float32

VM = pl.BlockSpec(memory_space=pltpu.VMEM)
SM = pl.BlockSpec(memory_space=pltpu.SMEM)
AN = pl.BlockSpec(memory_space=pl.ANY)


def held(x):
    return pltpu.with_memory_space_constraint(x, pltpu.VMEM)


def parked(x):
    return pltpu.with_memory_space_constraint(x, pltpu.HBM)


def contract(a, b, ca, cb):
    return lax.dot_general(a, b, (((ca,), (cb,)), ((), ())), preferred_element_type=F32)


def mebi(size):
    return size >> 20


def params(flops, mib):
    return dict(
        compiler_params=pltpu.CompilerParams(vmem_limit_bytes=int(mib * (1 << 20))),
        cost_estimate=pl.CostEstimate(flops=flops, transcendentals=0, bytes_accessed=1 << 20),
    )


def attention(queries, keys, values, new_keys, new_values, lengths, answers, routes, stops, o_proj, capacity, samples):
    _, _, steps, width = queries.shape
    table_rows = steps * samples
    slot_count = steps * capacity
    cache, kv_width = keys.shape[2:]
    kv_heads, heads = kv_width // HD, width // HD
    group = heads // kv_heads
    rows = group * steps
    first = cache - steps

    def body(
        q_ref,
        k_ref,
        v_ref,
        nk_ref,
        nv_ref,
        len_ref,
        ans_ref,
        routes_ref,
        stop_ref,
        o_hbm,
        out_ref,
        place_ref,
        expert_ref,
        active_ref,
        o_ref,
        q_s,
        a_s,
        used,
        sem,
    ):
        move = pltpu.make_async_copy(o_hbm, o_ref, sem)
        move.start()
        prompt = lax.axis_index("dp")
        slot_lane = lax.broadcasted_iota(jnp.int32, (1, E * slot_count), 1)
        expert_lane = lax.broadcasted_iota(jnp.int32, (1, LANES), 1)
        for i in range(steps * E):
            used[i] = 0
        for t in range(steps):
            active = jnp.full((samples, LANES), (1 - stop_ref[0, t]).astype(F32))
            active_ref[t * samples : (t + 1) * samples, :] = active

            def one(s, _):
                for k in range(TOP):
                    e = routes_ref[t, prompt, k, s]
                    place = used[t * E + e]
                    used[t * E + e] = place + 1
                    slot = e * slot_count + t * capacity + place
                    n = k * table_rows + t * samples + s
                    place_ref[pl.ds(n, 1), :] = (slot_lane == slot).astype(F32)
                    expert_ref[pl.ds(n, 1), :] = (expert_lane == e).astype(F32)
                return 0

            lax.fori_loop(0, samples, one, 0)
        for t in range(steps):
            q = q_ref[0, 0, t : t + 1, :].astype(F32)
            for h in range(heads):
                q_s[pl.ds(h * steps + t, 1), :] = q[:, h * HD : (h + 1) * HD]
        position = lax.broadcasted_iota(jnp.int32, (rows, cache), 1)
        step = lax.broadcasted_iota(jnp.int32, (rows, cache), 0) % steps
        fresh = position - first
        valid = (position < len_ref[0, 0]) | ((fresh >= 0) & (fresh <= step))
        new_keys = nk_ref[0, 0].astype(F32)
        new_values = nv_ref[0, 0].astype(F32)
        for k in range(kv_heads):
            at = slice(k * HD, (k + 1) * HD)
            q = q_s[k * rows : (k + 1) * rows, :]
            scores = contract(q.astype(BF), k_ref[0, 0, :, at], 1, 1)
            for u in range(steps):
                score = jnp.sum(q * new_keys[u : u + 1, at], -1, keepdims=True)
                scores = jnp.where(fresh == u, score, scores)
            scores = jnp.where(valid, scores * (HD**-0.5), -jnp.inf)
            e = jnp.exp(scores - jnp.max(scores, -1, keepdims=True))
            weights = (e / jnp.sum(e, -1, keepdims=True)).astype(BF)
            o = contract(jnp.where(fresh < 0, weights, jnp.zeros_like(weights)), v_ref[0, 0, :, at], 1, 0)
            weights = weights.astype(F32)
            for u in range(steps):
                weight = jnp.sum(jnp.where(fresh == u, weights, 0.0), -1, keepdims=True)
                o = o + weight * new_values[u : u + 1, at]
            for g in range(group):
                h = k * group + g
                a_s[:, h * HD : (h + 1) * HD] = o[g * steps : (g + 1) * steps, :]
        lane = lax.broadcasted_iota(jnp.int32, (1, ANSWERS), 1)
        for t in range(steps):
            a_s[t : t + 1, width:] = (lane == ans_ref[0, 0, t]).astype(F32)
        out_ref[...] = a_s[...].astype(BF)
        move.wait()

    return pl.pallas_call(
        body,
        in_specs=[VM, VM, VM, VM, VM, SM, SM, SM, SM, AN],
        out_specs=[VM] * 5,
        out_shape=[
            pltpu.VMEM((steps, width + ANSWERS), BF),
            jax.ShapeDtypeStruct((TOP * table_rows, E * slot_count), F32),
            jax.ShapeDtypeStruct((TOP * table_rows, LANES), F32),
            jax.ShapeDtypeStruct((table_rows, LANES), F32),
            pltpu.VMEM(o_proj.shape, o_proj.dtype),
        ],
        scratch_shapes=[
            pltpu.VMEM((heads * steps, HD), F32),
            pltpu.VMEM((steps, width + ANSWERS), F32),
            pltpu.SMEM((steps * E,), jnp.int32),
            pltpu.SemaphoreType.DMA,
        ],
        name="attention",
        **params(1 << 20, 2),
    )(
        *[parked(x) for x in (queries, keys, values, new_keys, new_values)],
        lengths,
        *[parked(x) for x in (answers, routes, stops, o_proj)],
    )


def repeated(payload, peers):
    def body(in_ref, out_ref):
        row = in_ref[...]
        for i in range(peers):
            out_ref[i] = row

    return pl.pallas_call(
        body,
        in_specs=[VM],
        out_specs=VM,
        out_shape=pltpu.VMEM((peers, *payload.shape), payload.dtype),
        name="repeated",
        **params(1 << 36, 2),
    )(held(payload))


def projection(recv, o_proj, residual, gain, router, places, experts, active, groups, spread):
    peers, steps, wide = recv.shape
    width = wide - ANSWERS
    columns = o_proj.shape[1]
    samples = residual.shape[2]
    rows = steps * samples
    slots = places.shape[1]
    slot_count = slots // E
    payload = columns + LANES

    def body(
        recv_ref,
        o_ref,
        res_ref,
        gain_ref,
        router_ref,
        place_ref,
        expert_ref,
        active_ref,
        out_ref,
        base_ref,
        pick_ref,
        vote_ref,
    ):
        x = jnp.concatenate([recv_ref[i] for i in range(peers)], 0)
        to = lax.broadcasted_iota(jnp.int32, (rows, rows), 0)
        at = lax.broadcasted_iota(jnp.int32, (rows, rows), 1)
        order = (at == (to % samples) * steps + to // samples).astype(BF)
        x = contract(order, x, 1, 0)
        tally = jnp.zeros((1, ANSWERS), F32)
        for t in range(steps):
            hits = jnp.sum(x[t * samples : (t + 1) * samples, width:], 0, keepdims=True)
            tally = tally + active_ref[t * samples : t * samples + 1, :] * hits
            vote_ref[t] = tally / jnp.maximum(jnp.sum(tally, -1, keepdims=True), 1.0)
        attn = contract(x[:, :width].astype(BF), o_ref[...], 1, 0)
        residual = jnp.concatenate([res_ref[t, 0].astype(F32) for t in range(steps)], 0)
        mixed = residual + attn
        active = active_ref[:, :1]
        base_ref[...] = residual + active * attn
        pick = place_ref[:rows, :]
        for k in range(1, TOP):
            pick = pick + place_ref[k * rows : (k + 1) * rows, :]
        pick_ref[...] = active * pick
        squares = jnp.sum(mixed * mixed, -1, keepdims=True)
        scaled = mixed * gain_ref[...]
        logits = lax.dot_general(
            scaled,
            router_ref[...],
            (((1,), (1,)), ((), ())),
            precision=lax.Precision.HIGHEST,
            preferred_element_type=F32,
        )
        hot = expert_ref[:, :E]
        difference = jnp.sum(logits * (hot[:rows] - hot[rows:]), -1, keepdims=True)
        lane = lax.broadcasted_iota(jnp.int32, (rows, LANES), 1)
        stacked = []
        for sign in (1.0, -1.0):
            stats = jnp.where(lane == 0, squares, jnp.where(lane == 1, sign * difference, 0.0))
            high = stats.astype(BF).astype(F32)
            rest = stats - high
            middle = rest.astype(BF).astype(F32)
            low = rest - middle
            stats = high + pltpu.roll(middle, 2, 1) + pltpu.roll(low, 4, 1)
            stacked.append(jnp.concatenate([scaled.astype(BF), stats.astype(BF)], 1))
        by_slot = contract(place_ref[...].astype(BF), jnp.concatenate(stacked, 0), 0, 0).astype(BF)
        for e in range(E):
            block = by_slot[e * slot_count : (e + 1) * slot_count, :]
            for group in range(groups):
                for copy in range(spread):
                    out_ref[group * E * spread + e * spread + copy] = block

    return pl.pallas_call(
        body,
        in_specs=[VM] * 8,
        out_specs=[VM] * 4,
        out_shape=[
            jax.ShapeDtypeStruct((groups * peers, slot_count, payload), BF),
            pltpu.VMEM((rows, columns), F32),
            pltpu.VMEM((rows, slots), F32),
            pltpu.VMEM((steps, 1, ANSWERS), F32),
        ],
        name="projection",
        **params(1 << 36, 2 + mebi(2 * groups * peers * slot_count * payload * 2)),
    )(recv, held(o_proj), held(residual), held(gain), held(router), places, experts, active)


def expert(recv, gate, up, down, peers, columns):
    groups = recv.shape[0] // peers
    slot_count = recv.shape[1]
    tokens = groups * slot_count
    width, hidden = gate.shape
    block = 512 if hidden % 512 == 0 else hidden
    blocks = hidden // block
    piece = 128 if block % 128 == 0 else block
    pieces = hidden // piece
    slots = min(5, pieces)

    def body(recv_ref, g_ref, u_ref, down_hbm, out_ref, x_s, d_s, acc_s, sems):
        def fetch(n):
            at = pl.ds(n * piece, piece)
            return pltpu.make_async_copy(down_hbm.at[0, at, :], d_s.at[n % slots], sems.at[n % slots])

        for n in range(slots):
            fetch(n).start()
        inverse, weight = [], []
        for i in range(groups):
            total = recv_ref[i * peers, :, columns:].astype(F32)
            for c in range(1, peers):
                total = total + recv_ref[i * peers + c, :, columns:].astype(F32)
            total = total + pltpu.roll(total, LANES - 2, 1) + pltpu.roll(total, LANES - 4, 1)
            inv = lax.rsqrt(total[:, 0:1] / width + EPSILON)
            inverse.append(inv)
            weight.append(1.0 / (1.0 + jnp.exp(-inv * total[:, 1:2])))
        inverse = jnp.concatenate(inverse, 0)
        weight = jnp.concatenate(weight, 0)
        for c in range(peers):
            x_s[:, c * columns : (c + 1) * columns] = jnp.concatenate(
                [recv_ref[i * peers + c, :, :columns] for i in range(groups)], 0
            )
        def hidden_of(i):
            at = slice(i * block, (i + 1) * block)
            g = contract(x_s[...], g_ref[:, at], 1, 0) * inverse
            u = contract(x_s[...], u_ref[:, at], 1, 0) * inverse
            return (g / (1.0 + jnp.exp(-g)) * u).astype(BF)

        state = hidden_of(0)
        for i in range(1, blocks + 1):
            after = hidden_of(i) if i < blocks else None
            for n in range((i - 1) * block // piece, i * block // piece):
                fetch(n).wait()
                at = n * piece - (i - 1) * block
                out = contract(state[:, at : at + piece], d_s[n % slots], 1, 0)
                acc_s[...] = out if n == 0 else acc_s[...] + out
                if n + slots < pieces:
                    fetch(n + slots).start()
            state = after
        for c in range(peers):
            mine = (acc_s[:, c * columns : (c + 1) * columns] * weight).astype(BF)
            for i in range(groups):
                out_ref[i * peers + c] = mine[i * slot_count : (i + 1) * slot_count, :]

    return pl.pallas_call(
        body,
        in_specs=[VM, VM, VM, AN],
        out_specs=VM,
        out_shape=pltpu.VMEM((groups * peers, slot_count, columns), BF),
        scratch_shapes=[
            pltpu.VMEM((tokens, width), BF),
            pltpu.VMEM((slots, piece, width), BF),
            pltpu.VMEM((tokens, width), F32),
            pltpu.SemaphoreType.DMA((slots,)),
        ],
        name="expert",
        **params(1 << 33, 4.5 + 2 * mebi(recv.size * 2 + tokens * width * 6)),
    )(held(recv), held(gate), held(up), parked(down))


def combine(recv, picks, base, votes, shape, groups, spread):
    steps, _, samples, columns = shape
    rows = steps * samples
    peers = E * spread

    def body(recv_ref, pick_ref, base_ref, vote_ref, out_ref, share_ref):
        share_ref[...] = vote_ref[...]
        pick = pick_ref[...].astype(BF)
        total = base_ref[...]
        for group in range(groups):
            for copy in range(spread):
                mine = jnp.concatenate([recv_ref[group * peers + e * spread + copy] for e in range(E)], 0)
                total = total + contract(pick, mine, 1, 0)
        for t in range(steps):
            out_ref[t, 0] = total[t * samples : (t + 1) * samples, :].astype(BF)

    return pl.pallas_call(
        body,
        in_specs=[VM] * 4,
        out_specs=[VM] * 2,
        out_shape=[jax.ShapeDtypeStruct(shape, BF), jax.ShapeDtypeStruct(votes.shape, F32)],
        name="combine",
        **params(1 << 26, 3 + mebi(2 * recv.size * 2)),
    )(recv, held(picks), held(base), held(votes))


def on_device(
    queries,
    cache_keys,
    cache_values,
    new_keys,
    new_values,
    cache_len,
    o_proj,
    residual_in,
    norm_gain,
    router,
    expert_gate,
    expert_up,
    expert_down,
    routes,
    answers,
    stop_mask,
):
    peers = lax.axis_size("expert")
    groups = lax.axis_size("dp")
    spread = peers // E
    samples, columns = residual_in.shape[2:]
    capacity = 2 * residual_in.shape[1] * samples * TOP // E
    gate, up = expert_gate.reshape(expert_gate.shape[1:]), expert_up.reshape(expert_up.shape[1:])
    payload, places, experts, active, o_v = attention(
        jnp.transpose(queries, (1, 2, 0, 3)),
        cache_keys,
        cache_values,
        jnp.transpose(new_keys, (1, 2, 0, 3)),
        jnp.transpose(new_values, (1, 2, 0, 3)),
        cache_len,
        jnp.transpose(answers, (1, 2, 0)),
        jnp.transpose(routes, (0, 1, 3, 2)),
        stop_mask.T,
        o_proj,
        capacity,
        samples,
    )
    recv = lax.all_to_all(repeated(payload, peers), "expert", split_axis=0, concat_axis=0, tiled=True)
    outgoing, base, picks, votes = projection(
        recv, o_v, residual_in, norm_gain.reshape(1, columns), router.T, places, experts, active, groups, spread
    )
    tokens = lax.all_to_all(outgoing, ("dp", "expert"), split_axis=0, concat_axis=0, tiled=True)
    partial = expert(tokens, gate, up, expert_down, peers, columns)
    returned = lax.all_to_all(partial, ("dp", "expert"), split_axis=0, concat_axis=0, tiled=True)
    updated, shares = combine(returned, picks, base, votes, residual_in.shape, groups, spread)
    return updated, shares


def solution(mesh):
    placed = (
        P(None, "dp", "expert", None),
        P("dp", "expert", None, None),
        P("dp", "expert", None, None),
        P(None, "dp", "expert", None),
        P(None, "dp", "expert", None),
        P("dp", "expert"),
        P(None, "expert"),
        P(None, "dp", None, "expert"),
        P("expert"),
        P("expert", None),
        P("expert", None, "dp"),
        P("expert", None, "dp"),
        P("expert", "dp", None),
        P(),
        P(None, "dp", "expert"),
        P(None, "dp"),
    )
    return jax.shard_map(
        on_device,
        mesh=mesh,
        in_specs=placed,
        out_specs=(P(None, "dp", None, "expert"), P(None, "dp", None)),
        check_vma=False,
    )
```
